768 devices in a mesh: group: 48 (over z, x), fsdp: 4 (over y_hi, core), tensor: 4 (over y_lo).
Axes of the slice: x: 4, y: 8 (y_hi: 2, y_lo: 4; y = y_hi * 4 + y_lo), z: 12, core: 2. Of those that a mesh axis runs over, the one named last changes fastest.
Arguments:
- tokens: bfloat16 [24576, 8192], P(('group', 'fsdp')), may hold values from -6 to 6
- cotangent: bfloat16 [24576, 512], P(('group', 'fsdp'), 'tensor'), may hold values from -0.0390625 to 0.0390625
- weight: bfloat16 [8192, 512], P('fsdp', 'tensor'), may hold values from -0.0625 to 0.0625
- moment_one: float32 [8192, 512], P('fsdp', 'tensor'), may hold values from -4 to 4
- moment_two: float32 [8192, 512], P('fsdp', 'tensor'), may hold values from 0.003 to 0.3
- hidden: bfloat16 [4, 12288, 8192], P(None, 'group', ('fsdp', 'tensor')), may hold values from -6 to 6
- queries: bfloat16 [4, 12288, 4096], P(None, ('group', 'fsdp', 'tensor')), may hold values from -145 to 145
- new_keys: bfloat16 [4, 12288, 512], P(None, ('group', 'fsdp', 'tensor')), may hold values from -4 to 4
- key_cache: bfloat16 [12288, 32, 512], P(('group', 'fsdp', 'tensor')), may hold values from -4 to 4
- value_cache: bfloat16 [12288, 32, 512], P(('group', 'fsdp', 'tensor')), may hold values from -6 to 6
- lengths: int32 [12288], P(('group', 'fsdp', 'tensor')), may hold values from 2 to 32
Outputs:
- new_weight: bfloat16 [8192, 512], P('fsdp', 'tensor')
- new_moment_one: float32 [8192, 512], P('fsdp', 'tensor')
- new_moment_two: float32 [8192, 512], P('fsdp', 'tensor')
- attention: bfloat16 [4, 12288, 4096], P(None, ('group', 'fsdp', 'tensor'))
The draws below stay inside these ranges and needn't reach their ends.
All inputs are finite; a program needn't handle non-finite values.
Results may differ from the reference program's by a relative error of at most 0.007.
Values may be sent and summed in bfloat16 or wider, within the bound.
No kernel may reach another device: no remote copies, remote signals or barrier semaphores. Data moves between devices by JAX's collectives and lax.ppermute only.
A program may use at most 64 MiB of HBM per device.

```python
import math
import jax
import jax.numpy as jnp
from jax import lax

D = 8192
HEAD_DIM = 128
GROUP_HEADS = 8
KV_HEADS = 4
STEPS = 4
ADAM_STEP = 10
ROW_DEV = 16
CACHE = 32
KVW = 512
QW = 4096
TOKENS = 24576
ROWS_ALL = 12288
N_GROUP = 48
N_FSDP = 4
N_TENSOR = 4


def joint_draw(key):
    base_key = jax.random.fold_in(key, 7)
    cached = jax.random.normal(jax.random.fold_in(base_key, 1), (ROWS_ALL, CACHE, KV_HEADS, HEAD_DIM), jnp.float32)
    cached = jnp.clip(cached, -4.0, 4.0)
    query_f = jax.random.normal(jax.random.fold_in(base_key, 2), (STEPS, ROWS_ALL, KV_HEADS, GROUP_HEADS, HEAD_DIM), jnp.float32)
    query_f = jnp.clip(query_f, -6.0, 6.0)
    return (cached.reshape(ROWS_ALL, CACHE, KVW), query_f.reshape(STEPS, ROWS_ALL, QW))


def draw_queries(key, part):
    return joint_draw(key)[1].astype(jnp.bfloat16)


def draw_key_cache(key, part):
    return joint_draw(key)[0].astype(jnp.bfloat16)


def touch_ends(entries, stream_key, least, top_value):
    extent = entries.shape
    place = [jax.random.randint(jax.random.fold_in(stream_key, axis), (), 0, extent[axis]) for axis in range(len(extent))]
    entries = entries.at[tuple(place)].set(least)
    longest = extent.index(max(extent))
    place[longest] = (place[longest] + 1) % extent[longest]
    return entries.at[tuple(place)].set(top_value)


def block_levels(rng, extent, cuts, smallest, high):
    def one(axis_at, blocks):
        draws = jax.random.uniform(jax.random.fold_in(jax.random.fold_in(rng, 6), axis_at), (blocks,), jnp.float32, smallest / len(cuts), high / len(cuts))
        return jnp.repeat(jnp.exp(draws), extent[axis_at] // blocks).reshape((-1,) + (1,) * (len(extent) - axis_at - 1))

    loudness = one(*cuts[0])
    for cut in cuts[1:]:
        loudness = loudness * one(*cut)
    return loudness


def centred(own_key, shape, width, limit, shards=(), kind=jnp.bfloat16):
    loudness = block_levels(own_key, shape, shards, -0.22, 0.18) if shards else 1.0
    entries = jax.random.normal(own_key, shape, jnp.float32) * width * loudness
    return jnp.minimum(jnp.maximum(entries, -limit), limit).astype(kind)


def setup_inputs(seed: int = 0) -> dict:
    key_list = jax.random.split(jax.random.key(seed), 12)
    return {
        "tokens": centred(key_list[0], (TOKENS, D), 1.0, 6.0, ((0, 192),)),
        "cotangent": centred(key_list[1], (TOKENS, KVW), TOKENS ** -0.5, 0.0390625, ((0, 192), (1, 4))),
        "weight": centred(key_list[2], (D, KVW), D ** -0.5, 0.0625, ((0, 4), (1, 4))),
        "moment_one": centred(key_list[3], (D, KVW), 1.0, 4.0, ((0, 4), (1, 4)), jnp.float32),
        "moment_two": jnp.clip(jnp.exp(math.log(0.3) - 4.6051702 * jax.random.uniform(key_list[4], (D, KVW), jnp.float32) ** block_levels(key_list[4], (D, KVW), ((0, 4), (1, 4)), -0.2, 0.2)), 0.003, 0.3),
        "hidden": centred(key_list[5], (STEPS, ROWS_ALL, D), 1.0, 6.0, ((1, 48), (2, 16))),
        "queries": draw_queries(jax.random.fold_in(key_list[11], 71), 0),
        "new_keys": centred(key_list[7], (STEPS, ROWS_ALL, KVW), 1.0, 4.0, ((1, 768),)),
        "key_cache": draw_key_cache(jax.random.fold_in(key_list[11], 71), 0),
        "value_cache": centred(key_list[9], (ROWS_ALL, CACHE, KVW), 1.0, 6.0, ((0, 768),)),
        "lengths": touch_ends(jax.random.randint(key_list[10], (ROWS_ALL,), 2, CACHE + 1), jax.random.fold_in(key_list[10], 1), 2, CACHE).astype(jnp.int32),
    }


learn_rate = 0.001
beta_one = 0.9
beta_two = 0.95
epsilon = 1e-08
decay_rate = 0.1
masked_score = -1e+30

def apply_adamw(gradient, weight, moment_one, moment_two):
    first_new = beta_one * moment_one + (1.0 - beta_one) * gradient
    second_new = beta_two * moment_two + (1.0 - beta_two) * gradient * gradient
    first_hat = first_new / (1.0 - beta_one ** ADAM_STEP)
    second_hat = second_new / (1.0 - beta_two ** ADAM_STEP)
    stepped = weight.astype(jnp.float32) * (1.0 - learn_rate * decay_rate) - learn_rate * first_hat / (jnp.sqrt(second_hat) + epsilon)
    return (stepped.astype(jnp.bfloat16), first_new, second_new)

def attend(queries, new_keys, fresh_values, key_cache, value_cache, lengths):
    row_total = lengths.shape[0]
    query_f = queries.reshape(STEPS, row_total, KV_HEADS, GROUP_HEADS, HEAD_DIM).astype(jnp.float32)
    cached_keys = key_cache.reshape(row_total, CACHE, KV_HEADS, HEAD_DIM).astype(jnp.float32)
    cached_values = value_cache.reshape(row_total, CACHE, KV_HEADS, HEAD_DIM).astype(jnp.float32)
    fresh_keys = new_keys.reshape(STEPS, row_total, KV_HEADS, HEAD_DIM).astype(jnp.float32)
    fresh_vals = fresh_values.reshape(STEPS, row_total, KV_HEADS, HEAD_DIM).astype(jnp.float32)
    score_scale = HEAD_DIM ** (-0.5)
    cached_scores = jnp.einsum('tnhjd,nphd->nhjtp', query_f, cached_keys) * score_scale
    fresh_scores = jnp.einsum('tnhjd,snhd->nhjts', query_f, fresh_keys) * score_scale
    cached_valid = jnp.arange(CACHE, dtype=jnp.int32)[None, :] < lengths[:, None]
    fresh_valid = jnp.arange(STEPS, dtype=jnp.int32)[None, :] <= jnp.arange(STEPS, dtype=jnp.int32)[:, None]
    cached_scores = jnp.where(cached_valid[:, None, None, None, :], cached_scores, masked_score)
    fresh_scores = jnp.where(fresh_valid[None, None, None, :, :], fresh_scores, masked_score)
    highest = jnp.maximum(lax.optimization_barrier(jnp.max(cached_scores, axis=-1)), lax.optimization_barrier(jnp.max(fresh_scores, axis=-1)))[..., None]
    cached_exp = jnp.exp(cached_scores - highest)
    fresh_exp = jnp.exp(fresh_scores - highest)
    denominator = lax.optimization_barrier(jnp.sum(cached_exp, axis=-1, keepdims=True)) + lax.optimization_barrier(jnp.sum(fresh_exp, axis=-1, keepdims=True))
    cached_probs = (cached_exp / denominator).astype(jnp.bfloat16).astype(jnp.float32)
    fresh_probs = (fresh_exp / denominator).astype(jnp.bfloat16).astype(jnp.float32)
    result = jnp.einsum('nhjtp,nphd->tnhjd', cached_probs, cached_values)
    result = result + jnp.einsum('nhjts,snhd->tnhjd', fresh_probs, fresh_vals)
    return result.reshape(STEPS, row_total, QW).astype(jnp.bfloat16)

def block_attend(packed):
    return attend(*packed)

def reference(tokens, cotangent, weight, moment_one, moment_two, hidden, queries, new_keys, key_cache, value_cache, lengths):
    gradient = lax.dot_general(tokens, cotangent, (((0,), (0,)), ((), ())), preferred_element_type=jnp.float32)
    new_weight, first_new, second_new = apply_adamw(gradient, weight, moment_one, moment_two)
    fresh = jnp.stack([jnp.dot(hidden[turn_index], new_weight, preferred_element_type=jnp.float32) for turn_index in range(STEPS)]).astype(jnp.bfloat16)
    group_rows = ROW_DEV * N_FSDP * N_TENSOR
    query_blocks = jnp.moveaxis(queries.reshape(STEPS, N_GROUP, group_rows, QW), 1, 0)
    key_blocks = jnp.moveaxis(new_keys.reshape(STEPS, N_GROUP, group_rows, KVW), 1, 0)
    fresh_blocks = jnp.moveaxis(fresh.reshape(STEPS, N_GROUP, group_rows, KVW), 1, 0)
    cache_keys = key_cache.reshape(N_GROUP, group_rows, CACHE, KVW)
    cache_values = value_cache.reshape(N_GROUP, group_rows, CACHE, KVW)
    length_blocks = lengths.reshape(N_GROUP, group_rows)
    outputs = lax.map(block_attend, (query_blocks, key_blocks, fresh_blocks, cache_keys, cache_values, length_blocks))
    attention = jnp.moveaxis(outputs, 0, 1).reshape(STEPS, ROWS_ALL, QW)
    return (new_weight, first_new, second_new, attention)
```

```python
import jax
import jax.numpy as jnp
from jax import lax
from jax.experimental import pallas as pl
from jax.experimental.pallas import tpu as pltpu
from jax.sharding import Mesh
from jax.sharding import PartitionSpec as P

HEAD_DIM = 128
GROUP_HEADS = 8
KV_HEADS = 4
STEPS = 4
ADAM_STEP = 10
GZ, GX, YH, YL, CO = "gz", "gx", "yh", "yl", "co"
GROUP = (GZ, GX)
FSDP = (YH, CO)
ALL = (GZ, GX, YH, CO, YL)
NX, NZ = 4, 12
QROWS = 512
PART = 48
STARTS = tuple(min(PART * k, QROWS - PART) for k in range(NZ))

learn_rate = 0.001
beta_one = 0.9
beta_two = 0.95
epsilon = 1e-08
decay_rate = 0.1
masked_score = -1e30


def apply_adamw(gradient, weight, moment_one, moment_two):
    first_new = beta_one * moment_one + (1.0 - beta_one) * gradient
    second_new = beta_two * moment_two + (1.0 - beta_two) * gradient * gradient
    first_hat = first_new / (1.0 - beta_one**ADAM_STEP)
    second_hat = second_new / (1.0 - beta_two**ADAM_STEP)
    stepped = weight.astype(jnp.float32) * (
        1.0 - learn_rate * decay_rate
    ) - learn_rate * first_hat / (jnp.sqrt(second_hat) + epsilon)
    return (stepped.astype(jnp.bfloat16), first_new, second_new)


def vmem(*shape_map):
    return pl.BlockSpec(memory_space=pltpu.VMEM)


def hbm():
    return pl.BlockSpec(memory_space=pl.ANY)


def pack_kernel(place, tokens, out, sems):
    other = 1 - place[0]
    copies = []
    for k in range(2):
        first = pl.multiple_of(k * 4096 + other * 2048, 2048)
        copies.append(
            pltpu.make_async_copy(
                tokens.at[:, pl.ds(first, 2048)], out.at[:, pl.ds(k * 2048, 2048)], sems.at[k]
            )
        )
    for c in copies:
        c.start()
    for c in copies:
        c.wait()


def pack_tokens(place, tokens):
    return pl.pallas_call(
        pack_kernel,
        out_shape=jax.ShapeDtypeStruct((128, 4096), jnp.bfloat16),
        in_specs=[pl.BlockSpec(memory_space=pltpu.SMEM), hbm()],
        out_specs=hbm(),
        scratch_shapes=[pltpu.SemaphoreType.DMA((2,))],
        name="pack_tokens",
    )(place, tokens)


def grad_kernel(place, own, recv, cot_own, cot_recv, out):
    t = place[1]
    cot = jnp.concatenate([cot_own[...], cot_recv[...]], axis=0)
    for k in range(NX):
        first = pl.multiple_of(((k + t) % NX) * QROWS, QROWS)
        tok = jnp.concatenate([own[:, pl.ds(first, QROWS)], recv[:, pl.ds(first, QROWS)]], axis=0)
        out[k, 0] = lax.dot_general(
            tok, cot, (((0,), (0,)), ((), ())), preferred_element_type=jnp.float32
        ).astype(jnp.bfloat16)


def partial_gradient(place, tokens, recv, cot_own, cot_recv):
    return pl.pallas_call(
        grad_kernel,
        out_shape=jax.ShapeDtypeStruct((NX, 2, QROWS, 128), jnp.bfloat16),
        grid_spec=pltpu.PrefetchScalarGridSpec(
            num_scalar_prefetch=1,
            grid=(2,),
            in_specs=[
                pl.BlockSpec((128, 2048), lambda i, p: (0, 2 * i + p[0])),
                pl.BlockSpec((128, 2048), lambda i, p: (0, i)),
                pl.BlockSpec((128, 128), lambda i, p: (0, 0)),
                pl.BlockSpec((128, 128), lambda i, p: (0, 0)),
            ],
            out_specs=pl.BlockSpec((NX, 1, QROWS, 128), lambda i, p: (0, i, 0, 0)),
        ),
        name="partial_gradient",
    )(place, tokens, recv, cot_own, cot_recv)


def sum_x_kernel(parts, out):
    for h in range(2):
        total = parts[0, h].astype(jnp.float32)
        for k in range(1, NX):
            total = total + parts[k, h].astype(jnp.float32)
        total = total.astype(jnp.bfloat16)
        for z in range(NZ):
            out[z, h] = total[STARTS[z] : STARTS[z] + PART]


def sum_over_x(parts):
    return pl.pallas_call(
        sum_x_kernel,
        out_shape=jax.ShapeDtypeStruct((NZ, 2, PART, 128), jnp.bfloat16),
        in_specs=[vmem()],
        out_specs=vmem(),
        name="sum_over_x",
    )(parts)


def shard_kernel(parts, weight, one, two, grad_out, weight_out):
    total = parts[0, 0].astype(jnp.float32)
    for z in range(NZ):
        for h in range(2):
            if z or h:
                total = total + parts[z, h].astype(jnp.float32)
    grad_out[...] = jnp.broadcast_to(total.astype(jnp.bfloat16)[None], grad_out.shape)
    weight_out[...] = apply_adamw(total, weight[...], one[...], two[...])[0]


def update_shard(parts, weight, one, two):
    return pl.pallas_call(
        shard_kernel,
        out_shape=(
            jax.ShapeDtypeStruct((NZ, PART, 128), jnp.bfloat16),
            jax.ShapeDtypeStruct((PART, 128), jnp.bfloat16),
        ),
        in_specs=[vmem()] * 4,
        out_specs=(vmem(), vmem()),
        name="update_shard",
    )(parts, weight, one, two)


def whole_quarter(parts):
    last = STARTS[NZ - 1]
    kept = [parts[k] for k in range(10)] + [parts[10][480 - last :]]
    return jnp.concatenate(kept, axis=0)


def join_kernel(parts, out):
    kept = [parts[k] for k in range(10)] + [parts[NZ - 2][480 - STARTS[NZ - 2] :]]
    whole = jnp.concatenate(kept, axis=0)
    for k in range(NX):
        out[k] = whole


def join_quarter(parts, name):
    return pl.pallas_call(
        join_kernel,
        out_shape=jax.ShapeDtypeStruct((NX, QROWS, 128), jnp.bfloat16),
        in_specs=[vmem()],
        out_specs=vmem(),
        name=name,
    )(parts)


def adamw_kernel(place, grad, weight, one, two, weight_out, one_out, two_out):
    new_weight, first, second = apply_adamw(
        grad[0].astype(jnp.float32), weight[...], one[...], two[...]
    )
    weight_out[...] = new_weight
    one_out[...] = first
    two_out[...] = second


def update_all(place, grad, weight, one, two):
    spot = lambda k, p: ((k + p[1]) % NX, 0)
    block = pl.BlockSpec((QROWS, 128), spot)
    shape = lambda d: jax.ShapeDtypeStruct((2048, 128), d)
    return pl.pallas_call(
        adamw_kernel,
        out_shape=(shape(jnp.bfloat16), shape(jnp.float32), shape(jnp.float32)),
        grid_spec=pltpu.PrefetchScalarGridSpec(
            num_scalar_prefetch=1,
            grid=(NX,),
            in_specs=[pl.BlockSpec((1, QROWS, 128), lambda k, p: (k, 0, 0)), block, block, block],
            out_specs=(block, block, block),
        ),
        name="update_all",
    )(place, grad, weight, one, two)


def joined_weight(place, parts, whole):
    t = place[1]
    for k in range(NX):
        first = pl.multiple_of(((t - k + NX) % NX) * 128, 128)
        whole[:, pl.ds(first, 128)] = parts[k]


def rows_times_weight(hidden, core, whole, out, extra):
    for s in range(STEPS):
        for h in range(2):
            value = jnp.dot(hidden[s, h, core], whole[...], preferred_element_type=jnp.float32)
            for l in range(4):
                piece = value[l * 16 : (l + 1) * 16]
                spot = h * 4 + l
                if extra is not None:
                    piece = piece + extra[spot, s * 16 : (s + 1) * 16].astype(jnp.float32)
                out[spot, s * 16 : (s + 1) * 16] = piece.astype(jnp.bfloat16)


def send_kernel(place, hidden, parts, out, whole):
    joined_weight(place, parts, whole)
    rows_times_weight(hidden, 1 - place[0], whole, out, None)


def keep_kernel(place, hidden, parts, recv, out, whole):
    joined_weight(place, parts, whole)
    rows_times_weight(hidden, place[0], whole, out, recv)


def values_part(place, hidden, parts, recv=None):
    args = (place, hidden, parts) + (() if recv is None else (recv,))
    return pl.pallas_call(
        send_kernel if recv is None else keep_kernel,
        out_shape=jax.ShapeDtypeStruct((8, STEPS * 16, 512), jnp.bfloat16),
        in_specs=[pl.BlockSpec(memory_space=pltpu.SMEM)] + [vmem()] * (len(args) - 1),
        out_specs=vmem(),
        scratch_shapes=[pltpu.VMEM((512, 512), jnp.bfloat16)],
        name="values_send" if recv is None else "values_keep",
    )(*args)


def attend_cached(queries, new_keys, key_cache, value_cache, lengths):
    row_total = lengths.shape[0]
    cache_len = key_cache.shape[1]
    query_b = queries.reshape(STEPS, row_total, KV_HEADS, GROUP_HEADS, HEAD_DIM)
    cached_keys = key_cache.reshape(row_total, cache_len, KV_HEADS, HEAD_DIM)
    cached_values = value_cache.reshape(row_total, cache_len, KV_HEADS, HEAD_DIM)
    fresh_keys = new_keys.reshape(STEPS, row_total, KV_HEADS, HEAD_DIM)
    score_scale = HEAD_DIM ** (-0.5)
    cached_scores = (
        jnp.einsum("tnhjd,nphd->nhjtp", query_b, cached_keys, preferred_element_type=jnp.float32)
        * score_scale
    )
    fresh_scores = (
        jnp.einsum("tnhjd,snhd->nhjts", query_b, fresh_keys, preferred_element_type=jnp.float32)
        * score_scale
    )
    cached_valid = jnp.arange(cache_len, dtype=jnp.int32)[None, :] < lengths[:, None]
    fresh_valid = (
        jnp.arange(STEPS, dtype=jnp.int32)[None, :] <= jnp.arange(STEPS, dtype=jnp.int32)[:, None]
    )
    cached_scores = jnp.where(cached_valid[:, None, None, None, :], cached_scores, masked_score)
    fresh_scores = jnp.where(fresh_valid[None, None, None, :, :], fresh_scores, masked_score)
    highest = jnp.maximum(jnp.max(cached_scores, axis=-1), jnp.max(fresh_scores, axis=-1))[
        ..., None
    ]
    cached_exp = jnp.exp(cached_scores - highest)
    fresh_exp = jnp.exp(fresh_scores - highest)
    denominator = jnp.sum(cached_exp, axis=-1, keepdims=True) + jnp.sum(
        fresh_exp, axis=-1, keepdims=True
    )
    cached_probs = (cached_exp / denominator).astype(jnp.bfloat16)
    fresh_probs = (fresh_exp / denominator).astype(jnp.bfloat16)
    result = jnp.einsum(
        "nhjtp,nphd->tnhjd", cached_probs, cached_values, preferred_element_type=jnp.float32
    )
    return result, fresh_probs


def attend_fresh(result, fresh_probs, fresh_values):
    row_total = result.shape[1]
    fresh_vals = fresh_values.reshape(STEPS, row_total, KV_HEADS, HEAD_DIM)
    result = result + jnp.einsum(
        "nhjts,snhd->tnhjd", fresh_probs, fresh_vals, preferred_element_type=jnp.float32
    )
    return result.reshape(STEPS, row_total, -1).astype(jnp.bfloat16)


def per_device(
    tokens,
    cotangent,
    weight,
    moment_one,
    moment_two,
    hidden,
    queries,
    new_keys,
    key_cache,
    value_cache,
    lengths,
):
    core, t = lax.axis_index(CO), lax.axis_index(YL)
    x, z = lax.axis_index(GX), lax.axis_index(GZ)
    place = jnp.stack([core, t]).astype(jnp.int32)
    swap = [(0, 1), (1, 0)]

    recv = lax.ppermute(pack_tokens(place, tokens), CO, swap)
    cot_recv = lax.ppermute(cotangent, CO, swap)
    parts = partial_gradient(place, tokens, recv, cotangent, cot_recv)
    parts = lax.all_to_all(parts, GX, 0, 0, tiled=True)
    parts = sum_over_x(parts).reshape(NZ * 2, PART, 128)
    parts = lax.all_to_all(parts, (GZ, YH), 0, 0, tiled=True).reshape(NZ, 2, PART, 128)

    first = ((x + t) % NX) * QROWS + jnp.minimum(PART * z, QROWS - PART)
    own = lambda a: lax.dynamic_slice_in_dim(a, first, PART, 0)
    grad_parts, shard = update_shard(parts, own(weight), own(moment_one), own(moment_two))

    turn = [(a * 4 + b, a * 4 + (a + b) % 4) for a in range(NX) for b in range(4)]
    shard = lax.ppermute(shard, (GX, YL), turn)
    weight_parts = lax.all_to_all(
        jnp.broadcast_to(shard[None], (NZ, PART, 128)), GZ, 0, 0, tiled=True
    )
    weight_parts = lax.all_to_all(join_quarter(weight_parts, "join_weight"), GX, 0, 0, tiled=True)

    hidden = hidden.reshape(STEPS, 2, 2, 64, 512)
    recv = lax.ppermute(values_part(place, hidden, weight_parts), CO, swap)
    values = values_part(place, hidden, weight_parts, recv)
    values = lax.all_to_all(values, (YH, YL), 0, 0, tiled=True)

    grad_parts = lax.all_to_all(grad_parts, GZ, 0, 0, tiled=True)
    grad_parts = lax.all_to_all(join_quarter(grad_parts, "join_grad"), GX, 0, 0, tiled=True)
    new_weight, first_new, second_new = update_all(
        place, grad_parts, weight, moment_one, moment_two
    )

    result, fresh_probs = attend_cached(queries, new_keys, key_cache, value_cache, lengths)
    fresh = jnp.sum(values.astype(jnp.float32), axis=0).astype(jnp.bfloat16)
    attention = attend_fresh(result, fresh_probs, fresh.reshape(STEPS, 16, 512))
    return (new_weight, first_new, second_new, attention)


def solution(mesh):
    split = Mesh(mesh.devices.reshape(NZ, NX, 2, 2, 4), (GZ, GX, YH, CO, YL))
    rows, cols = FSDP, YL
    return jax.shard_map(
        per_device,
        mesh=split,
        in_specs=(
            P(GROUP + FSDP, None),
            P(GROUP + FSDP, cols),
            P(rows, cols),
            P(rows, cols),
            P(rows, cols),
            P(None, GROUP, FSDP + (YL,)),
            P(None, ALL, None),
            P(None, ALL, None),
            P(ALL, None, None),
            P(ALL, None, None),
            P(ALL),
        ),
        out_specs=(P(rows, cols), P(rows, cols), P(rows, cols), P(None, ALL, None)),
        check_vma=False,
    )
```

```python
import jax
import jax.numpy as jnp
from jax import lax
from jax.experimental import pallas as pl
from jax.experimental.pallas import tpu as pltpu
from jax.sharding import Mesh
from jax.sharding import PartitionSpec as P

HEAD_DIM = 128
GROUP_HEADS = 8
KV_HEADS = 4
STEPS = 4
ADAM_STEP = 10
GZ, GX, YH, YL, CO = "gz", "gx", "yh", "yl", "co"
GROUP = (GZ, GX)
FSDP = (YH, CO)
ALL = (GZ, GX, YH, CO, YL)
NX, NZ = 4, 12
QROWS = 512
PART = 48
STARTS = tuple(min(PART * k, QROWS - PART) for k in range(NZ))

learn_rate = 0.001
beta_one = 0.9
beta_two = 0.95
epsilon = 1e-08
decay_rate = 0.1
masked_score = -1e30


def apply_adamw(gradient, weight, moment_one, moment_two):
    first_new = beta_one * moment_one + (1.0 - beta_one) * gradient
    second_new = beta_two * moment_two + (1.0 - beta_two) * gradient * gradient
    first_hat = first_new / (1.0 - beta_one**ADAM_STEP)
    second_hat = second_new / (1.0 - beta_two**ADAM_STEP)
    stepped = weight.astype(jnp.float32) * (
        1.0 - learn_rate * decay_rate
    ) - learn_rate * first_hat / (jnp.sqrt(second_hat) + epsilon)
    return (stepped.astype(jnp.bfloat16), first_new, second_new)


def vmem():
    return pl.BlockSpec(memory_space=pltpu.VMEM)


def wide(t):
    return t[0] // 2


def pack_kernel(t, tokens, out):
    out[...] = tokens[...]


def pack_tokens(t, tokens):
    return pl.pallas_call(
        pack_kernel,
        out_shape=jax.ShapeDtypeStruct((128, 4096), jnp.bfloat16),
        grid_spec=pltpu.PrefetchScalarGridSpec(
            num_scalar_prefetch=1,
            grid=(4,),
            in_specs=[pl.BlockSpec((128, 1024), lambda i, t: (0, 2 * i + wide(t)))],
            out_specs=pl.BlockSpec((128, 1024), lambda i, t: (0, i)),
        ),
        name="pack_tokens",
    )(t, tokens)


def grad_kernel(t, core, own_0, own_1, recv, cot_0, cot_1, out):
    b = t[0] % 2
    cot = jnp.concatenate([cot_0[...], cot_1[...]], axis=0)
    for rows, own in enumerate((own_0, own_1)):
        tok = jnp.concatenate([own[...], recv[:, rows * 1024 : (rows + 1) * 1024]], axis=0)
        value = lax.dot_general(
            tok, cot, (((0,), (0,)), ((), ())), preferred_element_type=jnp.float32
        ).astype(jnp.bfloat16)
        first = 2 * (core[0] ^ rows)
        out[first + b, 0] = value[:QROWS]
        out[first + (1 - b), 0] = value[QROWS:]


def partial_gradient(t, core, tokens, recv, cot_0, cot_1):
    return pl.pallas_call(
        grad_kernel,
        out_shape=jax.ShapeDtypeStruct((NX, 2, QROWS, 128), jnp.bfloat16),
        grid_spec=pltpu.PrefetchScalarGridSpec(
            num_scalar_prefetch=2,
            grid=(2,),
            in_specs=[
                pl.BlockSpec((128, 1024), lambda i, t, c: (0, 4 * i + wide(t))),
                pl.BlockSpec((128, 1024), lambda i, t, c: (0, 4 * i + 2 + wide(t))),
                pl.BlockSpec((128, 2048), lambda i, t, c: (0, i)),
                pl.BlockSpec((128, 128), lambda i, t, c: (0, 0)),
                pl.BlockSpec((128, 128), lambda i, t, c: (0, 0)),
            ],
            out_specs=pl.BlockSpec((NX, 1, QROWS, 128), lambda i, t, c: (0, i, 0, 0)),
        ),
        name="partial_gradient",
    )(t, core, tokens, tokens, recv, cot_0, cot_1)


def sum_x_kernel(parts, out):
    for h in range(2):
        total = parts[0, h].astype(jnp.float32)
        for k in range(1, NX):
            total = total + parts[k, h].astype(jnp.float32)
        total = total.astype(jnp.bfloat16)
        for z in range(NZ):
            out[z, h] = total[STARTS[z] : STARTS[z] + PART]


def sum_over_x(parts):
    return pl.pallas_call(
        sum_x_kernel,
        out_shape=jax.ShapeDtypeStruct((NZ, 2, PART, 128), jnp.bfloat16),
        in_specs=[vmem()],
        out_specs=vmem(),
        name="sum_over_x",
    )(parts)


def shard_kernel(parts, out):
    total = parts[0].astype(jnp.float32)
    for k in range(1, NZ * 2):
        total = total + parts[k].astype(jnp.float32)
    total = total.astype(jnp.bfloat16)
    for k in range(NZ * NX):
        out[k] = total


def sum_over_z(parts):
    return pl.pallas_call(
        shard_kernel,
        out_shape=jax.ShapeDtypeStruct((NZ * NX, PART, 128), jnp.bfloat16),
        in_specs=[vmem()],
        out_specs=vmem(),
        name="sum_over_z",
    )(parts)


def whole_block(parts, k):
    last = 480 - STARTS[NZ - 2]
    kept = [parts[z, k] for z in range(10)] + [parts[NZ - 2, k, last:]]
    return jnp.concatenate(kept, axis=0).astype(jnp.float32)


def adamw_kernel(t, core, back_0, back_1, weight, one, two, weight_out, one_out, two_out):
    for j, grad in enumerate((back_0, back_1)):

        @pl.when(pl.program_id(0) // 2 == j)
        def _():
            new_weight, first, second = apply_adamw(
                whole_block(grad, 0), weight[...], one[...], two[...]
            )
            weight_out[...] = new_weight
            one_out[...] = first
            two_out[...] = second


def update_all(t, core, back_0, back_1, weight, one, two):
    block = pl.BlockSpec(
        (QROWS, 128), lambda k, t, c: (t[0] ^ (2 * (c[0] ^ (k // 2))) ^ (k % 2), 0)
    )
    back = pl.BlockSpec((NZ, 1, PART, 128), lambda k, t, c: (0, k % 2, 0, 0))
    shape = lambda d: jax.ShapeDtypeStruct((2048, 128), d)
    return pl.pallas_call(
        adamw_kernel,
        out_shape=(shape(jnp.bfloat16), shape(jnp.float32), shape(jnp.float32)),
        grid_spec=pltpu.PrefetchScalarGridSpec(
            num_scalar_prefetch=2,
            grid=(NX,),
            in_specs=[back, back, block, block, block],
            out_specs=(block, block, block),
        ),
        name="update_all",
    )(t, core, back_0, back_1, weight, one, two)


def values_kernel(t, parts, state_0, state_1, own, near, far_own, far_near, out, whole):
    b = t[0] % 2

    @pl.when(pl.program_id(0) == 0)
    def _():
        for j, state in enumerate((state_0, state_1)):
            for i in range(2):
                rows = pl.ds(pl.multiple_of((b ^ i) * QROWS, QROWS), QROWS)
                p = 2 * j + i
                whole[p * QROWS : (p + 1) * QROWS] = apply_adamw(
                    whole_block(parts, p),
                    state[0, rows],
                    state[1, rows].astype(jnp.float32),
                    state[2, rows].astype(jnp.float32),
                )[0]

    value = None
    for p, rows in enumerate((own, near, far_own, far_near)):
        part = jnp.dot(
            rows[0], whole[p * QROWS : (p + 1) * QROWS], preferred_element_type=jnp.float32
        )
        value = part if value is None else value + part
    value = value.astype(jnp.bfloat16)
    for d in range(16):
        out[d] = value[d * 16 : (d + 1) * 16]


def values_part(t, parts, state_0, state_1, own, near, far_own, far_near):
    rows = pl.BlockSpec((1, 256, 512), lambda s, t: (s, 0, 0))
    state = pl.BlockSpec((3, 1024, 128), lambda s, t: (0, 0, 0))
    return pl.pallas_call(
        values_kernel,
        out_shape=jax.ShapeDtypeStruct((16, STEPS * 16, 128), jnp.bfloat16),
        grid_spec=pltpu.PrefetchScalarGridSpec(
            num_scalar_prefetch=1,
            grid=(STEPS,),
            in_specs=[
                pl.BlockSpec((NZ, NX, PART, 128), lambda s, t: (0, 0, 0, 0)),
                state,
                state,
                rows,
                rows,
                rows,
                rows,
            ],
            out_specs=pl.BlockSpec((16, 16, 128), lambda s, t: (0, s, 0)),
            scratch_shapes=[pltpu.VMEM((4 * QROWS, 128), jnp.bfloat16)],
        ),
        name="values_part",
    )(t, parts, state_0, state_1, own, near, far_own, far_near)


def attend_cached(queries, new_keys, key_cache, value_cache, lengths):
    row_total = lengths.shape[0]
    cache_len = key_cache.shape[1]
    query_b = queries.reshape(STEPS, row_total, KV_HEADS, GROUP_HEADS, HEAD_DIM)
    cached_keys = key_cache.reshape(row_total, cache_len, KV_HEADS, HEAD_DIM)
    cached_values = value_cache.reshape(row_total, cache_len, KV_HEADS, HEAD_DIM)
    fresh_keys = new_keys.reshape(STEPS, row_total, KV_HEADS, HEAD_DIM)
    score_scale = HEAD_DIM ** (-0.5)
    cached_scores = (
        jnp.einsum("tnhjd,nphd->nhjtp", query_b, cached_keys, preferred_element_type=jnp.float32)
        * score_scale
    )
    fresh_scores = (
        jnp.einsum("tnhjd,snhd->nhjts", query_b, fresh_keys, preferred_element_type=jnp.float32)
        * score_scale
    )
    cached_valid = jnp.arange(cache_len, dtype=jnp.int32)[None, :] < lengths[:, None]
    fresh_valid = (
        jnp.arange(STEPS, dtype=jnp.int32)[None, :] <= jnp.arange(STEPS, dtype=jnp.int32)[:, None]
    )
    cached_scores = jnp.where(cached_valid[:, None, None, None, :], cached_scores, masked_score)
    fresh_scores = jnp.where(fresh_valid[None, None, None, :, :], fresh_scores, masked_score)
    highest = jnp.maximum(jnp.max(cached_scores, axis=-1), jnp.max(fresh_scores, axis=-1))[
        ..., None
    ]
    cached_exp = jnp.exp(cached_scores - highest)
    fresh_exp = jnp.exp(fresh_scores - highest)
    denominator = jnp.sum(cached_exp, axis=-1, keepdims=True) + jnp.sum(
        fresh_exp, axis=-1, keepdims=True
    )
    cached_probs = (cached_exp / denominator).astype(jnp.bfloat16)
    fresh_probs = (fresh_exp / denominator).astype(jnp.bfloat16)
    result = jnp.einsum(
        "nhjtp,nphd->hjtnd", cached_probs, cached_values, preferred_element_type=jnp.float32
    ).reshape(KV_HEADS, -1, HEAD_DIM)
    spread = jnp.transpose(fresh_probs, (1, 2, 3, 0, 4))[..., None]
    same = jnp.eye(row_total, dtype=jnp.bool_)[None, None, None, :, None, :]
    spread = jnp.where(same, spread, jnp.zeros((), jnp.bfloat16))
    return result, spread.reshape(KV_HEADS, -1, STEPS * row_total)


def finish_kernel(values, result, spread, out):
    for h in range(KV_HEADS):
        total = None
        for k in range(2):
            for c in range(2):
                for v in (h & 1, (h & 1) + 2):
                    if (v ^ (2 * c)) == h:
                        part = values[k * 8 + c * 4 + v].astype(jnp.float32)
                        total = part if total is None else total + part
        value = result[h] + jnp.dot(
            spread[h], total.astype(jnp.bfloat16), preferred_element_type=jnp.float32
        )
        value = value.astype(jnp.bfloat16)
        for j in range(GROUP_HEADS):
            first = (h * GROUP_HEADS + j) * HEAD_DIM
            out[:, first : first + HEAD_DIM] = value[j * 64 : (j + 1) * 64]


def finish_attention(values, result, spread):
    return pl.pallas_call(
        finish_kernel,
        out_shape=jax.ShapeDtypeStruct((64, 4096), jnp.bfloat16),
        in_specs=[vmem()] * 3,
        out_specs=vmem(),
        name="finish_attention",
    )(values, result, spread)


def per_device(
    tokens,
    cotangent,
    weight,
    moment_one,
    moment_two,
    hidden,
    queries,
    new_keys,
    key_cache,
    value_cache,
    lengths,
):
    c, y = lax.axis_index(CO), lax.axis_index(YL)
    core, t = c.astype(jnp.int32).reshape(1), y.astype(jnp.int32).reshape(1)
    swap = [(0, 1), (1, 0)]
    spots = [(k, v) for k in range(2) for v in range(4)]
    bring = [[((k ^ j) * 4 + (v ^ (2 * k)), k * 4 + v) for k, v in spots] for j in range(2)]
    back = [[(d, s) for s, d in pairs] for pairs in bring]

    cots = [lax.ppermute(cotangent, (CO, YL), pairs) for pairs in bring]
    packed = pack_tokens(t, tokens)
    recv = lax.ppermute(packed, CO, swap)
    parts = partial_gradient(t, core, tokens, recv, *cots)
    near = lax.ppermute(hidden, YL, [(0, 1), (1, 0), (2, 3), (3, 2)])
    queries, new_keys, key_cache, value_cache, parts = lax.optimization_barrier(
        (queries, new_keys, key_cache, value_cache, parts)
    )
    states = []
    for j in range(2):
        first = ((y // 2) ^ c ^ j) * 1024
        states.append(
            jnp.stack(
                [
                    lax.dynamic_slice_in_dim(v, first, 1024, 0).astype(jnp.bfloat16)
                    for v in (weight, moment_one, moment_two)
                ]
            )
        )
    parts = lax.all_to_all(parts, GX, 0, 0, tiled=True)
    parts = sum_over_x(parts).reshape(NZ * 2, PART, 128)
    hidden, near, _ = lax.optimization_barrier((hidden, near, parts))
    parts = lax.all_to_all(parts, (GZ, YH), 0, 0, tiled=True)

    far = lax.ppermute(hidden, CO, swap)
    far_near = lax.ppermute(near, CO, swap)
    states = [lax.ppermute(v, (CO, YL), pairs) for v, pairs in zip(states, bring)]
    result, spread = attend_cached(queries, new_keys, key_cache, value_cache, lengths)
    parts, result, spread = lax.optimization_barrier((parts, result, spread))

    parts = sum_over_z(parts)
    grads = lax.all_to_all(parts, GROUP, 0, 0, tiled=True)
    grads = grads.reshape(NZ, NX, PART, 128)
    owned = [
        lax.ppermute(grads[:, 2 * j : 2 * j + 2], (CO, YL), back[j]) for j in range(2)
    ]
    values = values_part(t, grads, *states, hidden, near, far, far_near)
    values = lax.all_to_all(values, (YH, CO, YL), 0, 0, tiled=True)
    new_weight, first_new, second_new = update_all(t, core, *owned, weight, moment_one, moment_two)

    attention = finish_attention(values, result, spread).reshape(STEPS, 16, 4096)
    return (new_weight, first_new, second_new, attention)


def solution(mesh):
    split = Mesh(mesh.devices.reshape(NZ, NX, 2, 2, 4), (GZ, GX, YH, CO, YL))
    rows, cols = FSDP, YL
    return jax.shard_map(
        per_device,
        mesh=split,
        in_specs=(
            P(GROUP + FSDP, None),
            P(GROUP + FSDP, cols),
            P(rows, cols),
            P(rows, cols),
            P(rows, cols),
            P(None, GROUP, FSDP + (YL,)),
            P(None, ALL, None),
            P(None, ALL, None),
            P(ALL, None, None),
            P(ALL, None, None),
            P(ALL),
        ),
        out_specs=(P(rows, cols), P(rows, cols), P(rows, cols), P(None, ALL, None)),
        check_vma=False,
    )
```

```python
import jax
import jax.numpy as jnp
from jax import lax
from jax.experimental import pallas as pl
from jax.experimental.pallas import tpu as pltpu
from jax.sharding import Mesh
from jax.sharding import PartitionSpec as P

HEAD_DIM = 128
GROUP_HEADS = 8
KV_HEADS = 4
STEPS = 4
ADAM_STEP = 10
GZ, GX, YH, YL, CO = "gz", "gx", "yh", "yl", "co"
GROUP = (GZ, GX)
FSDP = (YH, CO)
ALL = (GZ, GX, YH, CO, YL)
NX, NZ = 4, 12
QROWS = 512
PART = 48
STARTS = tuple(min(PART * k, QROWS - PART) for k in range(NZ))

learn_rate = 0.001
beta_one = 0.9
beta_two = 0.95
epsilon = 1e-08
decay_rate = 0.1
masked_score = -1e30


def apply_adamw(gradient, weight, moment_one, moment_two):
    first_new = beta_one * moment_one + (1.0 - beta_one) * gradient
    second_new = beta_two * moment_two + (1.0 - beta_two) * gradient * gradient
    first_hat = first_new / (1.0 - beta_one**ADAM_STEP)
    second_hat = second_new / (1.0 - beta_two**ADAM_STEP)
    stepped = weight.astype(jnp.float32) * (
        1.0 - learn_rate * decay_rate
    ) - learn_rate * first_hat / (jnp.sqrt(second_hat) + epsilon)
    return (stepped.astype(jnp.bfloat16), first_new, second_new)


def vmem():
    return pl.BlockSpec(memory_space=pltpu.VMEM)


def wide(t):
    return t[0] // 2


def grad_kernel(t, core, own_0, own_1, recv_0, recv_1, cot_0, cot_1, out):
    b = t[0] % 2
    cot = jnp.concatenate([cot_0[...], cot_1[...]], axis=0)
    for rows, (own, recv) in enumerate(((own_0, recv_0), (own_1, recv_1))):
        tok = jnp.concatenate([own[...], recv[...]], axis=0)
        value = lax.dot_general(
            tok, cot, (((0,), (0,)), ((), ())), preferred_element_type=jnp.float32
        ).astype(jnp.bfloat16)
        first = 2 * (core[0] ^ rows)
        out[first + b, 0] = value[:QROWS]
        out[first + (1 - b), 0] = value[QROWS:]


def partial_gradient(t, core, tokens, recv, cot_0, cot_1):
    return pl.pallas_call(
        grad_kernel,
        out_shape=jax.ShapeDtypeStruct((NX, 2, QROWS, 128), jnp.bfloat16),
        grid_spec=pltpu.PrefetchScalarGridSpec(
            num_scalar_prefetch=2,
            grid=(2,),
            in_specs=[
                pl.BlockSpec((128, 1024), lambda i, t, c: (0, 4 * i + wide(t))),
                pl.BlockSpec((128, 1024), lambda i, t, c: (0, 4 * i + 2 + wide(t))),
                pl.BlockSpec((128, 1024), lambda i, t, c: (0, 4 * i + wide(t))),
                pl.BlockSpec((128, 1024), lambda i, t, c: (0, 4 * i + 2 + wide(t))),
                pl.BlockSpec((128, 128), lambda i, t, c: (0, 0)),
                pl.BlockSpec((128, 128), lambda i, t, c: (0, 0)),
            ],
            out_specs=pl.BlockSpec((NX, 1, QROWS, 128), lambda i, t, c: (0, i, 0, 0)),
        ),
        name="partial_gradient",
    )(t, core, tokens, tokens, recv, recv, cot_0, cot_1)


def sum_x_kernel(parts, out):
    for h in range(2):
        total = parts[0, h].astype(jnp.float32)
        for k in range(1, NX):
            total = total + parts[k, h].astype(jnp.float32)
        total = total.astype(jnp.bfloat16)
        for z in range(NZ):
            out[z, h] = total[STARTS[z] : STARTS[z] + PART]


def sum_over_x(parts):
    return pl.pallas_call(
        sum_x_kernel,
        out_shape=jax.ShapeDtypeStruct((NZ, 2, PART, 128), jnp.bfloat16),
        in_specs=[vmem()],
        out_specs=vmem(),
        name="sum_over_x",
    )(parts)


def shard_kernel(parts, state, grad_out, weight_out):
    total = parts[0].astype(jnp.float32)
    for k in range(1, NZ * 2):
        total = total + parts[k].astype(jnp.float32)
    grad_out[...] = total.astype(jnp.bfloat16)
    weight_out[...] = apply_adamw(total, state[0], state[1], state[2])[0]


def update_shard(parts, state):
    return pl.pallas_call(
        shard_kernel,
        out_shape=(jax.ShapeDtypeStruct((PART, 128), jnp.bfloat16),) * 2,
        in_specs=[vmem()] * 2,
        out_specs=(vmem(), vmem()),
        name="update_shard",
    )(parts, state)


def whole_block(parts, k):
    last = 480 - STARTS[NZ - 2]
    kept = [parts[z, k, 0] for z in range(10)] + [parts[NZ - 2, k, 0, last:]]
    return jnp.concatenate(kept, axis=0)


def adamw_kernel(t, core, grad, weight, one, two, weight_out, one_out, two_out):
    new_weight, first, second = apply_adamw(
        whole_block(grad, 0).astype(jnp.float32), weight[...], one[...], two[...]
    )
    weight_out[...] = new_weight
    one_out[...] = first
    two_out[...] = second


def update_all(t, core, both, weight, one, two):
    block = pl.BlockSpec(
        (QROWS, 128), lambda k, t, c: (t[0] ^ (2 * (c[0] ^ (k // 2))) ^ (k % 2), 0)
    )
    grad = pl.BlockSpec((NZ, 1, 1, PART, 128), lambda k, t, c: (0, k, 1, 0, 0))
    shape = lambda d: jax.ShapeDtypeStruct((2048, 128), d)
    return pl.pallas_call(
        adamw_kernel,
        out_shape=(shape(jnp.bfloat16), shape(jnp.float32), shape(jnp.float32)),
        grid_spec=pltpu.PrefetchScalarGridSpec(
            num_scalar_prefetch=2,
            grid=(NX,),
            in_specs=[grad, block, block, block],
            out_specs=(block, block, block),
        ),
        name="update_all",
    )(t, core, both, weight, one, two)


def values_kernel(parts, own, near, far_own, far_near, out, whole):
    @pl.when(pl.program_id(0) == 0)
    def _():
        for p in range(4):
            whole[p * QROWS : (p + 1) * QROWS] = whole_block(parts, p)

    value = None
    for p, rows in enumerate((own, near, far_own, far_near)):
        part = jnp.dot(
            rows[0], whole[p * QROWS : (p + 1) * QROWS], preferred_element_type=jnp.float32
        )
        value = part if value is None else value + part
    value = value.astype(jnp.bfloat16)
    for d in range(16):
        out[d] = value[d * 16 : (d + 1) * 16]


def values_part(both, own, near, far_own, far_near):
    rows = pl.BlockSpec((1, 256, 512), lambda s: (s, 0, 0))
    return pl.pallas_call(
        values_kernel,
        out_shape=jax.ShapeDtypeStruct((16, STEPS * 16, 128), jnp.bfloat16),
        grid=(STEPS,),
        in_specs=[
            pl.BlockSpec((NZ, NX, 1, PART, 128), lambda s: (0, 0, 0, 0, 0)),
            rows,
            rows,
            rows,
            rows,
        ],
        out_specs=pl.BlockSpec((16, 16, 128), lambda s: (0, s, 0)),
        scratch_shapes=[pltpu.VMEM((4 * QROWS, 128), jnp.bfloat16)],
        name="values_part",
    )(both, own, near, far_own, far_near)


def attend_cached(queries, new_keys, key_cache, lengths):
    row_total = lengths.shape[0]
    cache_len = key_cache.shape[1]
    query_b = queries.reshape(STEPS, row_total, KV_HEADS, GROUP_HEADS, HEAD_DIM)
    cached_keys = key_cache.reshape(row_total, cache_len, KV_HEADS, HEAD_DIM)
    fresh_keys = new_keys.reshape(STEPS, row_total, KV_HEADS, HEAD_DIM)
    score_scale = HEAD_DIM ** (-0.5)
    cached_scores = (
        jnp.einsum("tnhjd,nphd->nhjtp", query_b, cached_keys, preferred_element_type=jnp.float32)
        * score_scale
    )
    fresh_scores = (
        jnp.einsum("tnhjd,snhd->nhjts", query_b, fresh_keys, preferred_element_type=jnp.float32)
        * score_scale
    )
    cached_valid = jnp.arange(cache_len, dtype=jnp.int32)[None, :] < lengths[:, None]
    fresh_valid = (
        jnp.arange(STEPS, dtype=jnp.int32)[None, :] <= jnp.arange(STEPS, dtype=jnp.int32)[:, None]
    )
    cached_scores = jnp.where(cached_valid[:, None, None, None, :], cached_scores, masked_score)
    fresh_scores = jnp.where(fresh_valid[None, None, None, :, :], fresh_scores, masked_score)
    highest = jnp.maximum(jnp.max(cached_scores, axis=-1), jnp.max(fresh_scores, axis=-1))[
        ..., None
    ]
    cached_exp = jnp.exp(cached_scores - highest)
    fresh_exp = jnp.exp(fresh_scores - highest)
    denominator = jnp.sum(cached_exp, axis=-1, keepdims=True) + jnp.sum(
        fresh_exp, axis=-1, keepdims=True
    )
    cached_probs = (cached_exp / denominator).astype(jnp.bfloat16)
    fresh_probs = (fresh_exp / denominator).astype(jnp.bfloat16)
    return cached_probs, fresh_probs


def spread_probs(fresh_probs):
    row_total = fresh_probs.shape[0]
    spread = jnp.transpose(fresh_probs, (1, 2, 3, 0, 4))[..., None]
    same = jnp.eye(row_total, dtype=jnp.bool_)[None, None, None, :, None, :]
    spread = jnp.where(same, spread, jnp.zeros((), jnp.bfloat16))
    return spread.reshape(KV_HEADS, -1, STEPS * row_total)


def weigh_cached(cached_probs, value_cache):
    cached_values = value_cache.reshape(*value_cache.shape[:2], KV_HEADS, HEAD_DIM)
    return jnp.einsum(
        "nhjtp,nphd->hjtnd", cached_probs, cached_values, preferred_element_type=jnp.float32
    ).reshape(KV_HEADS, -1, HEAD_DIM)


def finish_kernel(first_0, first_1, second_0, second_1, result, spread, out):
    total = None
    for piece in (first_0, first_1, second_0, second_1):
        part = piece[0].astype(jnp.float32)
        total = part if total is None else total + part
    value = result[0] + jnp.dot(
        spread[0], total.astype(jnp.bfloat16), preferred_element_type=jnp.float32
    )
    value = value.astype(jnp.bfloat16)
    for j in range(GROUP_HEADS):
        out[:, j * HEAD_DIM : (j + 1) * HEAD_DIM] = value[j * 64 : (j + 1) * 64]


def finish_attention(values, result, spread):
    source = lambda k, c: pl.BlockSpec(
        (1, 64, 128), lambda h: (k * 8 + c * 4 + (h ^ (2 * c)), 0, 0)
    )
    return pl.pallas_call(
        finish_kernel,
        out_shape=jax.ShapeDtypeStruct((64, 4096), jnp.bfloat16),
        grid=(KV_HEADS,),
        in_specs=[
            source(0, 0),
            source(0, 1),
            source(1, 0),
            source(1, 1),
            pl.BlockSpec((1, 512, 128), lambda h: (h, 0, 0)),
            pl.BlockSpec((1, 512, 64), lambda h: (h, 0, 0)),
        ],
        out_specs=pl.BlockSpec((64, 1024), lambda h: (0, h)),
        name="finish_attention",
    )(values, values, values, values, result, spread)


def per_device(
    tokens,
    cotangent,
    weight,
    moment_one,
    moment_two,
    hidden,
    queries,
    new_keys,
    key_cache,
    value_cache,
    lengths,
):
    c, y = lax.axis_index(CO), lax.axis_index(YL)
    x, z = lax.axis_index(GX), lax.axis_index(GZ)
    core, t = c.astype(jnp.int32).reshape(1), y.astype(jnp.int32).reshape(1)
    swap = [(0, 1), (1, 0)]
    spots = [(k, v) for k in range(2) for v in range(4)]
    bring = [[((k ^ j) * 4 + (v ^ (2 * k)), k * 4 + v) for k, v in spots] for j in range(2)]

    cots = [lax.ppermute(cotangent, (CO, YL), pairs) for pairs in bring]
    recv = lax.ppermute(tokens, CO, swap)
    parts = partial_gradient(t, core, tokens, recv, *cots)
    queries, new_keys, key_cache, parts = lax.optimization_barrier(
        (queries, new_keys, key_cache, parts)
    )
    parts = lax.all_to_all(parts, GX, 0, 0, tiled=True)
    near = lax.ppermute(hidden, YL, [(0, 1), (1, 0), (2, 3), (3, 2)])

    j, i = x // 2, x % 2
    first = (y ^ (2 * (c ^ j)) ^ i) * QROWS + jnp.minimum(PART * z, QROWS - PART)
    state = jnp.stack(
        [
            lax.dynamic_slice_in_dim(v, first, PART, 0).astype(jnp.float32)
            for v in (weight, moment_one, moment_two)
        ]
    )
    turn = [(v * 8 + s, v * 8 + d) for v in range(NX) for s, d in bring[v // 2]]
    back = [(d, s) for s, d in turn]
    state = lax.ppermute(state, (GX, CO, YL), turn)

    parts = sum_over_x(parts).reshape(NZ * 2, PART, 128)
    parts = lax.all_to_all(parts, (GZ, YH), 0, 0, tiled=True)
    probs = attend_cached(queries, new_keys, key_cache, lengths)
    parts, state, probs = lax.optimization_barrier((parts, state, probs))
    grad, shard = update_shard(parts, state)

    grad = lax.ppermute(grad, (GX, CO, YL), back)
    both = jnp.broadcast_to(jnp.stack([shard, grad])[None], (NZ * NX, 2, PART, 128))
    both = lax.all_to_all(both, GROUP, 0, 0, tiled=True)
    both = both.reshape(NZ, NX, 2, PART, 128)
    far = lax.ppermute(hidden, CO, swap)
    far_near = lax.ppermute(near, CO, swap)
    cached_probs, fresh_probs = probs
    result = weigh_cached(cached_probs, value_cache)
    spread = spread_probs(fresh_probs)

    both, result, spread = lax.optimization_barrier((both, result, spread))
    values = values_part(both, hidden, near, far, far_near)
    values = lax.all_to_all(values, (YH, CO, YL), 0, 0, tiled=True)
    new_weight, first_new, second_new = update_all(t, core, both, weight, moment_one, moment_two)
    attention = finish_attention(values, result, spread).reshape(STEPS, 16, 4096)
    return (new_weight, first_new, second_new, attention)


def solution(mesh):
    split = Mesh(mesh.devices.reshape(NZ, NX, 2, 2, 4), (GZ, GX, YH, CO, YL))
    rows, cols = FSDP, YL
    return jax.shard_map(
        per_device,
        mesh=split,
        in_specs=(
            P(GROUP + FSDP, None),
            P(GROUP + FSDP, cols),
            P(rows, cols),
            P(rows, cols),
            P(rows, cols),
            P(None, GROUP, FSDP + (YL,)),
            P(None, ALL, None),
            P(None, ALL, None),
            P(ALL, None, None),
            P(ALL, None, None),
            P(ALL),
        ),
        out_specs=(P(rows, cols), P(rows, cols), P(rows, cols), P(None, ALL, None)),
        check_vma=False,
    )
```

```python
import jax
import jax.numpy as jnp
from jax import lax
from jax.experimental import pallas as pl
from jax.experimental.pallas import tpu as pltpu
from jax.sharding import Mesh
from jax.sharding import PartitionSpec as P

HEAD_DIM = 128
GROUP_HEADS = 8
KV_HEADS = 4
STEPS = 4
ADAM_STEP = 10
GZ, GX, YH, YL, CO = "gz", "gx", "yh", "yl", "co"
GROUP = (GZ, GX)
FSDP = (YH, CO)
ALL = (GZ, GX, YH, CO, YL)
NX, NZ = 4, 12
QROWS = 512
PART = 48
STARTS = tuple(min(PART * k, QROWS - PART) for k in range(NZ))

learn_rate = 0.001
beta_one = 0.9
beta_two = 0.95
epsilon = 1e-08
decay_rate = 0.1
masked_score = -1e30


def apply_adamw(gradient, weight, moment_one, moment_two):
    first_new = beta_one * moment_one + (1.0 - beta_one) * gradient
    second_new = beta_two * moment_two + (1.0 - beta_two) * gradient * gradient
    first_hat = first_new / (1.0 - beta_one**ADAM_STEP)
    second_hat = second_new / (1.0 - beta_two**ADAM_STEP)
    stepped = weight.astype(jnp.float32) * (
        1.0 - learn_rate * decay_rate
    ) - learn_rate * first_hat / (jnp.sqrt(second_hat) + epsilon)
    return (stepped.astype(jnp.bfloat16), first_new, second_new)


def vmem():
    return pl.BlockSpec(memory_space=pltpu.VMEM)


def wide(t):
    return t[0] // 2


def grad_kernel(t, core, own_0, own_1, recv_0, recv_1, cot_0, cot_1, out):
    b = t[0] % 2
    cot = jnp.concatenate([cot_0[...], cot_1[...]], axis=0)
    for rows, (own, recv) in enumerate(((own_0, recv_0), (own_1, recv_1))):
        tok = jnp.concatenate([own[...], recv[...]], axis=0)
        value = lax.dot_general(
            tok, cot, (((0,), (0,)), ((), ())), preferred_element_type=jnp.float32
        ).astype(jnp.bfloat16)
        first = 2 * (core[0] ^ rows)
        out[first + b, 0] = value[:QROWS]
        out[first + (1 - b), 0] = value[QROWS:]


def partial_gradient(t, core, tokens, recv, cot_0, cot_1):
    return pl.pallas_call(
        grad_kernel,
        out_shape=jax.ShapeDtypeStruct((NX, 2, QROWS, 128), jnp.bfloat16),
        grid_spec=pltpu.PrefetchScalarGridSpec(
            num_scalar_prefetch=2,
            grid=(2,),
            in_specs=[
                pl.BlockSpec((128, 1024), lambda i, t, c: (0, 4 * i + wide(t))),
                pl.BlockSpec((128, 1024), lambda i, t, c: (0, 4 * i + 2 + wide(t))),
                pl.BlockSpec((128, 1024), lambda i, t, c: (0, 4 * i + wide(t))),
                pl.BlockSpec((128, 1024), lambda i, t, c: (0, 4 * i + 2 + wide(t))),
                pl.BlockSpec((128, 128), lambda i, t, c: (0, 0)),
                pl.BlockSpec((128, 128), lambda i, t, c: (0, 0)),
            ],
            out_specs=pl.BlockSpec((NX, 1, QROWS, 128), lambda i, t, c: (0, i, 0, 0)),
        ),
        name="partial_gradient",
    )(t, core, tokens, tokens, recv, recv, cot_0, cot_1)


def sum_x_kernel(parts, out):
    total = parts[0].astype(jnp.float32)
    for k in range(1, NX * 2):
        total = total + parts[k].astype(jnp.float32)
    total = total.astype(jnp.bfloat16)
    for z in range(NZ):
        out[z] = total[STARTS[z] : STARTS[z] + PART]


def sum_over_x(parts):
    return pl.pallas_call(
        sum_x_kernel,
        out_shape=jax.ShapeDtypeStruct((NZ, PART, 128), jnp.bfloat16),
        in_specs=[vmem()],
        out_specs=vmem(),
        name="sum_over_x",
    )(parts)


def shard_kernel(parts, state, grad_out, weight_out):
    total = parts[0].astype(jnp.float32)
    for k in range(1, NZ):
        total = total + parts[k].astype(jnp.float32)
    grad_out[...] = total.astype(jnp.bfloat16)
    weight_out[...] = apply_adamw(total, state[0], state[1], state[2])[0]


def update_shard(parts, state):
    return pl.pallas_call(
        shard_kernel,
        out_shape=(jax.ShapeDtypeStruct((PART, 128), jnp.bfloat16),) * 2,
        in_specs=[vmem()] * 2,
        out_specs=(vmem(), vmem()),
        name="update_shard",
    )(parts, state)


def join_kernel(parts, out):
    last = 480 - STARTS[NZ - 2]
    for kind in range(2):
        kept = [parts[z, kind] for z in range(10)] + [parts[NZ - 2, kind, last:]]
        whole = jnp.concatenate(kept, axis=0)
        for k in range(NX):
            out[k, kind] = whole


def join_parts(parts):
    return pl.pallas_call(
        join_kernel,
        out_shape=jax.ShapeDtypeStruct((NX, 2, QROWS, 128), jnp.bfloat16),
        in_specs=[vmem()],
        out_specs=vmem(),
        name="join_parts",
    )(parts)


def adamw_kernel(t, core, grad, weight, one, two, weight_out, one_out, two_out):
    new_weight, first, second = apply_adamw(
        grad[0, 0].astype(jnp.float32), weight[...], one[...], two[...]
    )
    weight_out[...] = new_weight
    one_out[...] = first
    two_out[...] = second


def update_all(t, core, both, weight, one, two):
    block = pl.BlockSpec(
        (QROWS, 128), lambda k, t, c: (t[0] ^ (2 * (c[0] ^ (k // 2))) ^ (k % 2), 0)
    )
    grad = pl.BlockSpec((1, 1, QROWS, 128), lambda k, t, c: (k, 1, 0, 0))
    shape = lambda d: jax.ShapeDtypeStruct((2048, 128), d)
    return pl.pallas_call(
        adamw_kernel,
        out_shape=(shape(jnp.bfloat16), shape(jnp.float32), shape(jnp.float32)),
        grid_spec=pltpu.PrefetchScalarGridSpec(
            num_scalar_prefetch=2,
            grid=(NX,),
            in_specs=[grad, block, block, block],
            out_specs=(block, block, block),
        ),
        name="update_all",
    )(t, core, both, weight, one, two)


def values_kernel(parts, own, near, far_own, far_near, out):
    value = None
    for p, rows in enumerate((own, near, far_own, far_near)):
        part = jnp.dot(rows[0], parts[p, 0], preferred_element_type=jnp.float32)
        value = part if value is None else value + part
    value = value.astype(jnp.bfloat16)
    for d in range(16):
        out[d] = value[d * 16 : (d + 1) * 16]


def values_part(both, own, near, far_own, far_near):
    rows = pl.BlockSpec((1, 256, 512), lambda s: (s, 0, 0))
    return pl.pallas_call(
        values_kernel,
        out_shape=jax.ShapeDtypeStruct((16, STEPS * 16, 128), jnp.bfloat16),
        grid=(STEPS,),
        in_specs=[
            pl.BlockSpec((NX, 1, QROWS, 128), lambda s: (0, 0, 0, 0)),
            rows,
            rows,
            rows,
            rows,
        ],
        out_specs=pl.BlockSpec((16, 16, 128), lambda s: (0, s, 0)),
        name="values_part",
    )(both, own, near, far_own, far_near)


def attend_cached(queries, new_keys, key_cache, lengths):
    row_total = lengths.shape[0]
    cache_len = key_cache.shape[1]
    query_b = queries.reshape(STEPS, row_total, KV_HEADS, GROUP_HEADS, HEAD_DIM)
    cached_keys = key_cache.reshape(row_total, cache_len, KV_HEADS, HEAD_DIM)
    fresh_keys = new_keys.reshape(STEPS, row_total, KV_HEADS, HEAD_DIM)
    score_scale = HEAD_DIM ** (-0.5)
    cached_scores = (
        jnp.einsum("tnhjd,nphd->nhjtp", query_b, cached_keys, preferred_element_type=jnp.float32)
        * score_scale
    )
    fresh_scores = (
        jnp.einsum("tnhjd,snhd->nhjts", query_b, fresh_keys, preferred_element_type=jnp.float32)
        * score_scale
    )
    cached_valid = jnp.arange(cache_len, dtype=jnp.int32)[None, :] < lengths[:, None]
    fresh_valid = (
        jnp.arange(STEPS, dtype=jnp.int32)[None, :] <= jnp.arange(STEPS, dtype=jnp.int32)[:, None]
    )
    cached_scores = jnp.where(cached_valid[:, None, None, None, :], cached_scores, masked_score)
    fresh_scores = jnp.where(fresh_valid[None, None, None, :, :], fresh_scores, masked_score)
    highest = jnp.maximum(jnp.max(cached_scores, axis=-1), jnp.max(fresh_scores, axis=-1))[
        ..., None
    ]
    cached_exp = jnp.exp(cached_scores - highest)
    fresh_exp = jnp.exp(fresh_scores - highest)
    denominator = jnp.sum(cached_exp, axis=-1, keepdims=True) + jnp.sum(
        fresh_exp, axis=-1, keepdims=True
    )
    cached_probs = (cached_exp / denominator).astype(jnp.bfloat16)
    fresh_probs = (fresh_exp / denominator).astype(jnp.bfloat16)
    return cached_probs, fresh_probs


def spread_probs(fresh_probs):
    row_total = fresh_probs.shape[0]
    spread = jnp.transpose(fresh_probs, (1, 2, 3, 0, 4))[..., None]
    same = jnp.eye(row_total, dtype=jnp.bool_)[None, None, None, :, None, :]
    spread = jnp.where(same, spread, jnp.zeros((), jnp.bfloat16))
    return spread.reshape(KV_HEADS, -1, STEPS * row_total)


def weigh_cached(cached_probs, value_cache):
    cached_values = value_cache.reshape(*value_cache.shape[:2], KV_HEADS, HEAD_DIM)
    return jnp.einsum(
        "nhjtp,nphd->hjtnd", cached_probs, cached_values, preferred_element_type=jnp.float32
    ).reshape(KV_HEADS, -1, HEAD_DIM)


def finish_kernel(values, result, spread, out):
    for h in range(KV_HEADS):
        total = None
        for k in range(2):
            for c in range(2):
                for v in (h & 1, (h & 1) + 2):
                    if (v ^ (2 * c)) == h:
                        part = values[k * 8 + c * 4 + v].astype(jnp.float32)
                        total = part if total is None else total + part
        value = result[h] + jnp.dot(
            spread[h], total.astype(jnp.bfloat16), preferred_element_type=jnp.float32
        )
        value = value.astype(jnp.bfloat16)
        for j in range(GROUP_HEADS):
            first = (h * GROUP_HEADS + j) * HEAD_DIM
            out[:, first : first + HEAD_DIM] = value[j * 64 : (j + 1) * 64]


def finish_attention(values, result, spread):
    return pl.pallas_call(
        finish_kernel,
        out_shape=jax.ShapeDtypeStruct((64, 4096), jnp.bfloat16),
        in_specs=[vmem()] * 3,
        out_specs=vmem(),
        name="finish_attention",
    )(values, result, spread)


def per_device(
    tokens,
    cotangent,
    weight,
    moment_one,
    moment_two,
    hidden,
    queries,
    new_keys,
    key_cache,
    value_cache,
    lengths,
):
    c, y = lax.axis_index(CO), lax.axis_index(YL)
    x, z = lax.axis_index(GX), lax.axis_index(GZ)
    core, t = c.astype(jnp.int32).reshape(1), y.astype(jnp.int32).reshape(1)
    swap = [(0, 1), (1, 0)]
    spots = [(k, v) for k in range(2) for v in range(4)]
    bring = [[((k ^ j) * 4 + (v ^ (2 * k)), k * 4 + v) for k, v in spots] for j in range(2)]

    cots = [lax.ppermute(cotangent, (CO, YL), pairs) for pairs in bring]
    recv = lax.ppermute(tokens, CO, swap)
    parts = partial_gradient(t, core, tokens, recv, *cots)
    early = (weight, moment_one, moment_two)
    queries, new_keys, key_cache, early, parts = lax.optimization_barrier(
        (queries, new_keys, key_cache, early, parts)
    )
    parts = lax.all_to_all(parts.reshape(NX * 2, QROWS, 128), (GX, YH), 0, 0, tiled=True)

    j, i = x // 2, x % 2
    first = (y ^ (2 * (c ^ j)) ^ i) * QROWS + jnp.minimum(PART * z, QROWS - PART)
    state = jnp.stack(
        [lax.dynamic_slice_in_dim(v, first, PART, 0).astype(jnp.float32) for v in early]
    )
    turn = [(v * 8 + s, v * 8 + d) for v in range(NX) for s, d in bring[v // 2]]
    back = [(d, s) for s, d in turn]
    state = lax.ppermute(state, (GX, CO, YL), turn)

    far = lax.ppermute(hidden, CO, swap)
    cached_probs, fresh_probs = attend_cached(queries, new_keys, key_cache, lengths)
    spread = spread_probs(fresh_probs)
    parts = sum_over_x(parts)
    parts = lax.all_to_all(parts, GZ, 0, 0, tiled=True)
    parts, state, cached_probs, spread = lax.optimization_barrier(
        (parts, state, cached_probs, spread)
    )
    grad, shard = update_shard(parts, state)

    grad = lax.ppermute(grad, (GX, CO, YL), back)
    both = jnp.broadcast_to(jnp.stack([shard, grad])[None], (NZ, 2, PART, 128))
    both = lax.all_to_all(both, GZ, 0, 0, tiled=True)
    near = lax.ppermute(hidden, YL, [(0, 1), (1, 0), (2, 3), (3, 2)])
    result = weigh_cached(cached_probs, value_cache)
    both = join_parts(both)
    both = lax.all_to_all(both, GX, 0, 0, tiled=True)
    far_near = lax.ppermute(near, CO, swap)
    both, result = lax.optimization_barrier((both, result))
    values = values_part(both, hidden, near, far, far_near)
    values = lax.all_to_all(values, (YH, CO, YL), 0, 0, tiled=True)
    new_weight, first_new, second_new = update_all(t, core, both, weight, moment_one, moment_two)
    attention = finish_attention(values, result, spread).reshape(STEPS, 16, 4096)
    return (new_weight, first_new, second_new, attention)


def solution(mesh):
    split = Mesh(mesh.devices.reshape(NZ, NX, 2, 2, 4), (GZ, GX, YH, CO, YL))
    rows, cols = FSDP, YL
    return jax.shard_map(
        per_device,
        mesh=split,
        in_specs=(
            P(GROUP + FSDP, None),
            P(GROUP + FSDP, cols),
            P(rows, cols),
            P(rows, cols),
            P(rows, cols),
            P(None, GROUP, FSDP + (YL,)),
            P(None, ALL, None),
            P(None, ALL, None),
            P(ALL, None, None),
            P(ALL, None, None),
            P(ALL),
        ),
        out_specs=(P(rows, cols), P(rows, cols), P(rows, cols), P(None, ALL, None)),
        check_vma=False,
    )
```

```python
import jax
import jax.numpy as jnp
from jax import lax
from jax.experimental import pallas as pl
from jax.experimental.pallas import tpu as pltpu
from jax.sharding import Mesh
from jax.sharding import PartitionSpec as P

HEAD_DIM = 128
GROUP_HEADS = 8
KV_HEADS = 4
STEPS = 4
ADAM_STEP = 10
GZ, GX, YH, YL, CO = "gz", "gx", "yh", "yl", "co"
GROUP = (GZ, GX)
FSDP = (YH, CO)
ALL = (GZ, GX, YH, CO, YL)
NX, NZ = 4, 12
QROWS = 512
PART = 48
STARTS = tuple(min(PART * k, QROWS - PART) for k in range(NZ))

learn_rate = 0.001
beta_one = 0.9
beta_two = 0.95
epsilon = 1e-08
decay_rate = 0.1
masked_score = -1e30


def apply_adamw(gradient, weight, moment_one, moment_two):
    first_new = beta_one * moment_one + (1.0 - beta_one) * gradient
    second_new = beta_two * moment_two + (1.0 - beta_two) * gradient * gradient
    first_hat = first_new / (1.0 - beta_one**ADAM_STEP)
    second_hat = second_new / (1.0 - beta_two**ADAM_STEP)
    stepped = weight.astype(jnp.float32) * (
        1.0 - learn_rate * decay_rate
    ) - learn_rate * first_hat / (jnp.sqrt(second_hat) + epsilon)
    return (stepped.astype(jnp.bfloat16), first_new, second_new)


def vmem():
    return pl.BlockSpec(memory_space=pltpu.VMEM)


def wide(t):
    return t[0] // 2


def grad_kernel(t, core, own_0, own_1, recv_0, recv_1, cot_0, cot_1, out):
    b = t[0] % 2
    cot = jnp.concatenate([cot_0[...], cot_1[...]], axis=0)
    for rows, (own, recv) in enumerate(((own_0, recv_0), (own_1, recv_1))):
        tok = jnp.concatenate([own[...], recv[...]], axis=0)
        value = lax.dot_general(
            tok, cot, (((0,), (0,)), ((), ())), preferred_element_type=jnp.float32
        ).astype(jnp.bfloat16)
        first = 2 * (core[0] ^ rows)
        out[first + b, 0] = value[:QROWS]
        out[first + (1 - b), 0] = value[QROWS:]


def partial_gradient(t, core, tokens, recv, cot_0, cot_1):
    return pl.pallas_call(
        grad_kernel,
        out_shape=jax.ShapeDtypeStruct((NX, 2, QROWS, 128), jnp.bfloat16),
        grid_spec=pltpu.PrefetchScalarGridSpec(
            num_scalar_prefetch=2,
            grid=(2,),
            in_specs=[
                pl.BlockSpec((128, 1024), lambda i, t, c: (0, 4 * i + wide(t))),
                pl.BlockSpec((128, 1024), lambda i, t, c: (0, 4 * i + 2 + wide(t))),
                pl.BlockSpec((128, 1024), lambda i, t, c: (0, 4 * i + wide(t))),
                pl.BlockSpec((128, 1024), lambda i, t, c: (0, 4 * i + 2 + wide(t))),
                pl.BlockSpec((128, 128), lambda i, t, c: (0, 0)),
                pl.BlockSpec((128, 128), lambda i, t, c: (0, 0)),
            ],
            out_specs=pl.BlockSpec((NX, 1, QROWS, 128), lambda i, t, c: (0, i, 0, 0)),
        ),
        name="partial_gradient",
    )(t, core, tokens, tokens, recv, recv, cot_0, cot_1)


def sum_x_kernel(parts, out):
    for h in range(2):
        total = parts[0, h].astype(jnp.float32)
        for k in range(1, NX):
            total = total + parts[k, h].astype(jnp.float32)
        total = total.astype(jnp.bfloat16)
        for z in range(NZ):
            out[z, h] = total[STARTS[z] : STARTS[z] + PART]


def sum_over_x(parts):
    return pl.pallas_call(
        sum_x_kernel,
        out_shape=jax.ShapeDtypeStruct((NZ, 2, PART, 128), jnp.bfloat16),
        in_specs=[vmem()],
        out_specs=vmem(),
        name="sum_over_x",
    )(parts)


def shard_kernel(parts, state, grad_out, weight_out):
    total = parts[0].astype(jnp.float32)
    for k in range(1, NZ * 2):
        total = total + parts[k].astype(jnp.float32)
    grad_out[...] = total.astype(jnp.bfloat16)
    weight_out[...] = apply_adamw(total, state[0], state[1], state[2])[0]


def update_shard(parts, state):
    return pl.pallas_call(
        shard_kernel,
        out_shape=(jax.ShapeDtypeStruct((PART, 128), jnp.bfloat16),) * 2,
        in_specs=[vmem()] * 2,
        out_specs=(vmem(), vmem()),
        name="update_shard",
    )(parts, state)


def join_kernel(parts, out):
    last = 480 - STARTS[NZ - 2]
    for kind in range(2):
        kept = [parts[z, kind] for z in range(10)] + [parts[NZ - 2, kind, last:]]
        whole = jnp.concatenate(kept, axis=0)
        for k in range(NX):
            out[k, kind] = whole


def join_parts(parts):
    return pl.pallas_call(
        join_kernel,
        out_shape=jax.ShapeDtypeStruct((NX, 2, QROWS, 128), jnp.bfloat16),
        in_specs=[vmem()],
        out_specs=vmem(),
        name="join_parts",
    )(parts)


def adamw_kernel(t, core, grad, weight, one, two, weight_out, one_out, two_out):
    new_weight, first, second = apply_adamw(
        grad[0, 0].astype(jnp.float32), weight[...], one[...], two[...]
    )
    weight_out[...] = new_weight
    one_out[...] = first
    two_out[...] = second


def update_all(t, core, both, weight, one, two):
    block = pl.BlockSpec(
        (QROWS, 128), lambda k, t, c: (t[0] ^ (2 * (c[0] ^ (k // 2))) ^ (k % 2), 0)
    )
    grad = pl.BlockSpec((1, 1, QROWS, 128), lambda k, t, c: (k, 1, 0, 0))
    shape = lambda d: jax.ShapeDtypeStruct((2048, 128), d)
    return pl.pallas_call(
        adamw_kernel,
        out_shape=(shape(jnp.bfloat16), shape(jnp.float32), shape(jnp.float32)),
        grid_spec=pltpu.PrefetchScalarGridSpec(
            num_scalar_prefetch=2,
            grid=(NX,),
            in_specs=[grad, block, block, block],
            out_specs=(block, block, block),
        ),
        name="update_all",
    )(t, core, both, weight, one, two)


def values_kernel(parts, own, near, far_own, far_near, out):
    value = None
    for p, rows in enumerate((own, near, far_own, far_near)):
        part = jnp.dot(rows[0], parts[p, 0], preferred_element_type=jnp.float32)
        value = part if value is None else value + part
    value = value.astype(jnp.bfloat16)
    for d in range(16):
        out[d] = value[d * 16 : (d + 1) * 16]


def values_part(both, own, near, far_own, far_near):
    rows = pl.BlockSpec((1, 256, 512), lambda s: (s, 0, 0))
    return pl.pallas_call(
        values_kernel,
        out_shape=jax.ShapeDtypeStruct((16, STEPS * 16, 128), jnp.bfloat16),
        grid=(STEPS,),
        in_specs=[
            pl.BlockSpec((NX, 1, QROWS, 128), lambda s: (0, 0, 0, 0)),
            rows,
            rows,
            rows,
            rows,
        ],
        out_specs=pl.BlockSpec((16, 16, 128), lambda s: (0, s, 0)),
        name="values_part",
    )(both, own, near, far_own, far_near)


def attend_cached(queries, new_keys, key_cache, lengths):
    row_total = lengths.shape[0]
    cache_len = key_cache.shape[1]
    query_b = queries.reshape(STEPS, row_total, KV_HEADS, GROUP_HEADS, HEAD_DIM)
    cached_keys = key_cache.reshape(row_total, cache_len, KV_HEADS, HEAD_DIM)
    fresh_keys = new_keys.reshape(STEPS, row_total, KV_HEADS, HEAD_DIM)
    score_scale = HEAD_DIM ** (-0.5)
    cached_scores = (
        jnp.einsum("tnhjd,nphd->nhjtp", query_b, cached_keys, preferred_element_type=jnp.float32)
        * score_scale
    )
    fresh_scores = (
        jnp.einsum("tnhjd,snhd->nhjts", query_b, fresh_keys, preferred_element_type=jnp.float32)
        * score_scale
    )
    cached_valid = jnp.arange(cache_len, dtype=jnp.int32)[None, :] < lengths[:, None]
    fresh_valid = (
        jnp.arange(STEPS, dtype=jnp.int32)[None, :] <= jnp.arange(STEPS, dtype=jnp.int32)[:, None]
    )
    cached_scores = jnp.where(cached_valid[:, None, None, None, :], cached_scores, masked_score)
    fresh_scores = jnp.where(fresh_valid[None, None, None, :, :], fresh_scores, masked_score)
    highest = jnp.maximum(jnp.max(cached_scores, axis=-1), jnp.max(fresh_scores, axis=-1))[
        ..., None
    ]
    cached_exp = jnp.exp(cached_scores - highest)
    fresh_exp = jnp.exp(fresh_scores - highest)
    denominator = jnp.sum(cached_exp, axis=-1, keepdims=True) + jnp.sum(
        fresh_exp, axis=-1, keepdims=True
    )
    cached_probs = (cached_exp / denominator).astype(jnp.bfloat16)
    fresh_probs = (fresh_exp / denominator).astype(jnp.bfloat16)
    return cached_probs, fresh_probs


def spread_probs(fresh_probs):
    row_total = fresh_probs.shape[0]
    spread = jnp.transpose(fresh_probs, (1, 2, 3, 0, 4))[..., None]
    same = jnp.eye(row_total, dtype=jnp.bool_)[None, None, None, :, None, :]
    spread = jnp.where(same, spread, jnp.zeros((), jnp.bfloat16))
    return spread.reshape(KV_HEADS, -1, STEPS * row_total)


def weigh_cached(cached_probs, value_cache):
    cached_values = value_cache.reshape(*value_cache.shape[:2], KV_HEADS, HEAD_DIM)
    return jnp.einsum(
        "nhjtp,nphd->hjtnd", cached_probs, cached_values, preferred_element_type=jnp.float32
    ).reshape(KV_HEADS, -1, HEAD_DIM)


def finish_kernel(values, result, spread, out):
    for h in range(KV_HEADS):
        total = None
        for k in range(2):
            for c in range(2):
                for v in (h & 1, (h & 1) + 2):
                    if (v ^ (2 * c)) == h:
                        part = values[k * 8 + c * 4 + v].astype(jnp.float32)
                        total = part if total is None else total + part
        value = result[h] + jnp.dot(
            spread[h], total.astype(jnp.bfloat16), preferred_element_type=jnp.float32
        )
        value = value.astype(jnp.bfloat16)
        for j in range(GROUP_HEADS):
            first = (h * GROUP_HEADS + j) * HEAD_DIM
            out[:, first : first + HEAD_DIM] = value[j * 64 : (j + 1) * 64]


def finish_attention(values, result, spread):
    return pl.pallas_call(
        finish_kernel,
        out_shape=jax.ShapeDtypeStruct((64, 4096), jnp.bfloat16),
        in_specs=[vmem()] * 3,
        out_specs=vmem(),
        name="finish_attention",
    )(values, result, spread)


def per_device(
    tokens,
    cotangent,
    weight,
    moment_one,
    moment_two,
    hidden,
    queries,
    new_keys,
    key_cache,
    value_cache,
    lengths,
):
    c, y = lax.axis_index(CO), lax.axis_index(YL)
    x, z = lax.axis_index(GX), lax.axis_index(GZ)
    core, t = c.astype(jnp.int32).reshape(1), y.astype(jnp.int32).reshape(1)
    swap = [(0, 1), (1, 0)]
    spots = [(k, v) for k in range(2) for v in range(4)]
    bring = [[((k ^ j) * 4 + (v ^ (2 * k)), k * 4 + v) for k, v in spots] for j in range(2)]

    cots = [lax.ppermute(cotangent, (CO, YL), pairs) for pairs in bring]
    recv = lax.ppermute(tokens, CO, swap)
    parts = partial_gradient(t, core, tokens, recv, *cots)
    early = (weight, moment_one, moment_two)
    queries, new_keys, key_cache, early, parts = lax.optimization_barrier(
        (queries, new_keys, key_cache, early, parts)
    )
    parts = lax.all_to_all(parts, GX, 0, 0, tiled=True)

    j, i = x // 2, x % 2
    first = (y ^ (2 * (c ^ j)) ^ i) * QROWS + jnp.minimum(PART * z, QROWS - PART)
    state = jnp.stack(
        [lax.dynamic_slice_in_dim(v, first, PART, 0).astype(jnp.float32) for v in early]
    )
    turn = [(v * 8 + s, v * 8 + d) for v in range(NX) for s, d in bring[v // 2]]
    back = [(d, s) for s, d in turn]
    state = lax.ppermute(state, (GX, CO, YL), turn)

    near = lax.ppermute(hidden, YL, [(0, 1), (1, 0), (2, 3), (3, 2)])
    parts = sum_over_x(parts).reshape(NZ * 2, PART, 128)
    parts = lax.all_to_all(parts, (GZ, YH), 0, 0, tiled=True)
    far = lax.ppermute(hidden, CO, swap)
    far_near = lax.ppermute(near, CO, swap)
    cached_probs, fresh_probs = attend_cached(queries, new_keys, key_cache, lengths)
    spread = spread_probs(fresh_probs)
    parts, state, cached_probs, spread = lax.optimization_barrier(
        (parts, state, cached_probs, spread)
    )
    grad, shard = update_shard(parts, state)

    grad = lax.ppermute(grad, (GX, CO, YL), back)
    both = jnp.broadcast_to(jnp.stack([shard, grad])[None], (NZ, 2, PART, 128))
    both = lax.all_to_all(both, GZ, 0, 0, tiled=True)
    result = weigh_cached(cached_probs, value_cache)
    both, far, far_near = lax.optimization_barrier((both, far, far_near))
    both = join_parts(both)
    both = lax.all_to_all(both, GX, 0, 0, tiled=True)
    both, result = lax.optimization_barrier((both, result))
    values = values_part(both, hidden, near, far, far_near)
    values = lax.all_to_all(values, (YH, CO, YL), 0, 0, tiled=True)
    new_weight, first_new, second_new = update_all(t, core, both, weight, moment_one, moment_two)
    attention = finish_attention(values, result, spread).reshape(STEPS, 16, 4096)
    return (new_weight, first_new, second_new, attention)


def solution(mesh):
    split = Mesh(mesh.devices.reshape(NZ, NX, 2, 2, 4), (GZ, GX, YH, CO, YL))
    rows, cols = FSDP, YL
    return jax.shard_map(
        per_device,
        mesh=split,
        in_specs=(
            P(GROUP + FSDP, None),
            P(GROUP + FSDP, cols),
            P(rows, cols),
            P(rows, cols),
            P(rows, cols),
            P(None, GROUP, FSDP + (YL,)),
            P(None, ALL, None),
            P(None, ALL, None),
            P(ALL, None, None),
            P(ALL, None, None),
            P(ALL),
        ),
        out_specs=(P(rows, cols), P(rows, cols), P(rows, cols), P(None, ALL, None)),
        check_vma=False,
    )
```
